16 devices in a mesh: dp: 4 (over z, y), sp: 4 (over x, core).
Axes of the slice: x: 2, y: 2, z: 2, core: 2. Of those that a mesh axis runs over, the one named last changes fastest.
Arguments:
- tokens: bfloat16 [1024, 2048], P(('dp', 'sp')), parts along dimension 0
- w_query: bfloat16 [2048, 2048], replicated
- w_key: bfloat16 [2048, 2048], replicated
- w_value: bfloat16 [2048, 2048], replicated
- w_out: bfloat16 [2048, 2048], replicated
- w_gate: bfloat16 [2048, 2048], replicated
- w_up: bfloat16 [2048, 2048], replicated
- w_down: bfloat16 [2048, 2048], replicated
- w_router: bfloat16 [2048, 60], replicated
- expert_ids: int32 [1024, 4], P(('dp', 'sp')), parts along dimension 0
Outputs:
- output 1: bfloat16 [1024, 2048], P(('dp', 'sp')), parts along dimension 0
- output 2: bfloat16 [240, 32, 2048], P(('dp', 'sp')), parts along dimension 0
There are 4 independent parts. The reference program is written for one: setup_inputs(seed, part) draws one part's arguments, and reference() takes and returns one part's arrays. A program takes and returns all parts, laid end to end along the dimension named above; an argument that names none is the same for every part.
All inputs are finite; a program needn't handle non-finite values.
Results may differ from the reference program's by a relative error of at most 0.00521.
Values are sent between devices in bfloat16 or wider.
A program may use at most 1 GiB of HBM per device.

```python
import math
import jax
import jax.numpy as jnp
from jax import lax

HIDDEN = 2048
Q_HEADS = 16
KV_HEADS = 16
HEAD_DIM = 128
N_EXPERTS = 60
TOP_K = 4
GROUP_SIZE = 4
TOKENS_DEV = 64
CAPACITY = 8

SEQ_LEN = GROUP_SIZE * TOKENS_DEV
Q_WIDTH = Q_HEADS * HEAD_DIM
KV_WIDTH = KV_HEADS * HEAD_DIM
GQA_RATIO = Q_HEADS // KV_HEADS
QUERY_BLOCK = min(SEQ_LEN, 16)
BUF_ROWS = N_EXPERTS * GROUP_SIZE * CAPACITY


def normal_weight(rng_key, rows, cols, gain):
    w_scale = gain / math.sqrt(rows)
    return (jax.random.normal(rng_key, (rows, cols), jnp.float32) * w_scale).astype(jnp.bfloat16)


def draw_routing(rng_key):
    bits_key, hot_key = jax.random.split(rng_key)
    noise_bits = jax.random.randint(bits_key, (SEQ_LEN, N_EXPERTS), 0, 65536)
    expert_range = jnp.arange(N_EXPERTS, dtype=jnp.int32)
    scores = noise_bits * N_EXPERTS + expert_range[None, :]
    hot_expert = jnp.repeat(jax.random.randint(hot_key, (GROUP_SIZE,), 0, N_EXPERTS), TOKENS_DEV)
    local_pos = jnp.arange(SEQ_LEN, dtype=jnp.int32) % TOKENS_DEV
    forced = (local_pos[:, None] < CAPACITY) & (hot_expert[:, None] == expert_range[None, :])
    scores = scores + forced.astype(jnp.int32) * (65536 * N_EXPERTS)
    return lax.top_k(scores, TOP_K)[1].astype(jnp.int32)


def setup_inputs(seed: int = 0, part: int = 0) -> dict:
    base_key = jax.random.key(seed)
    w_keys = jax.random.split(base_key, 8)
    part_keys = jax.random.split(jax.random.fold_in(base_key, part), 2)
    score_gain = math.sqrt(max(1.0, math.log(SEQ_LEN / 8.0)))
    tokens = jax.random.normal(part_keys[0], (SEQ_LEN, HIDDEN), jnp.float32).astype(jnp.bfloat16)
    return {
        'tokens': tokens,
        'w_query': normal_weight(w_keys[0], HIDDEN, Q_WIDTH, score_gain),
        'w_key': normal_weight(w_keys[1], HIDDEN, KV_WIDTH, 1.0),
        'w_value': normal_weight(w_keys[2], HIDDEN, KV_WIDTH, 1.0),
        'w_out': normal_weight(w_keys[3], Q_WIDTH, HIDDEN, 2.0),
        'w_gate': normal_weight(w_keys[4], HIDDEN, HIDDEN, 1.0),
        'w_up': normal_weight(w_keys[5], HIDDEN, HIDDEN, 1.0),
        'w_down': normal_weight(w_keys[6], HIDDEN, HIDDEN, 1.0),
        'w_router': normal_weight(w_keys[7], HIDDEN, N_EXPERTS, 1.0),
        'expert_ids': draw_routing(part_keys[1]),
    }


def attention(queries, keys_bf, values_bf):
    queries_f32 = queries.astype(jnp.float32).reshape(SEQ_LEN // QUERY_BLOCK, QUERY_BLOCK, KV_HEADS, GQA_RATIO, HEAD_DIM)
    keys_f32 = keys_bf.astype(jnp.float32).reshape(SEQ_LEN, KV_HEADS, HEAD_DIM)
    values_f32 = values_bf.astype(jnp.float32).reshape(SEQ_LEN, KV_HEADS, HEAD_DIM)
    key_pos = jnp.arange(SEQ_LEN, dtype=jnp.int32)
    inv_scale = 1.0 / math.sqrt(HEAD_DIM)

    def one_block(blk_args):
        q_blk, q_start = blk_args
        scores = jnp.einsum('qkgd,skd->kgqs', q_blk, keys_f32) * inv_scale
        query_pos = q_start + jnp.arange(QUERY_BLOCK, dtype=jnp.int32)
        scores = jnp.where(query_pos[:, None] >= key_pos[None, :], scores, -jnp.inf)
        attn_probs = jax.nn.softmax(scores, axis=-1).astype(jnp.bfloat16).astype(jnp.float32)
        blk_out = jnp.einsum('kgqs,skd->qkgd', attn_probs, values_f32)
        return blk_out.astype(jnp.bfloat16).reshape(QUERY_BLOCK, Q_WIDTH)

    starts = jnp.arange(SEQ_LEN // QUERY_BLOCK, dtype=jnp.int32) * QUERY_BLOCK
    return lax.map(one_block, (queries_f32, starts)).reshape(SEQ_LEN, Q_WIDTH)


def dispatch(hidden, w_router, expert_ids):
    logits = jnp.dot(hidden, w_router, preferred_element_type=jnp.float32)
    gate_vals = jax.nn.sigmoid(jnp.take_along_axis(logits, expert_ids, axis=1))
    pair_expert = expert_ids.reshape(GROUP_SIZE, TOKENS_DEV * TOP_K)
    onehot = (pair_expert[:, :, None] == jnp.arange(N_EXPERTS, dtype=jnp.int32)[None, None, :]).astype(jnp.int32)
    slot_rank = jnp.sum((jnp.cumsum(onehot, axis=1) - onehot) * onehot, axis=2)
    source = jnp.arange(GROUP_SIZE, dtype=jnp.int32)[:, None]
    dest_row = jnp.where(slot_rank < CAPACITY, (pair_expert * GROUP_SIZE + source) * CAPACITY + slot_rank, BUF_ROWS).reshape(-1)
    pair_token = jnp.arange(SEQ_LEN * TOP_K, dtype=jnp.int32) // TOP_K
    slot_token = jnp.zeros((BUF_ROWS,), jnp.int32).at[dest_row].set(pair_token, mode='drop')
    slot_gate = jnp.zeros((BUF_ROWS,), jnp.float32).at[dest_row].set(gate_vals.reshape(-1), mode='drop')
    gathered = hidden[slot_token].astype(jnp.float32) * slot_gate[:, None]
    return gathered.astype(jnp.bfloat16).reshape(N_EXPERTS, GROUP_SIZE * CAPACITY, HIDDEN)


def reference(tokens, w_query, w_key, w_value, w_out, w_gate, w_up, w_down, w_router, expert_ids):
    queries = jnp.dot(tokens, w_query, preferred_element_type=jnp.float32).astype(jnp.bfloat16)
    keys_bf = jnp.dot(tokens, w_key, preferred_element_type=jnp.float32).astype(jnp.bfloat16)
    values_bf = jnp.dot(tokens, w_value, preferred_element_type=jnp.float32).astype(jnp.bfloat16)
    attn_out = attention(queries, keys_bf, values_bf)
    hidden = (tokens.astype(jnp.float32) + jnp.dot(attn_out, w_out, preferred_element_type=jnp.float32)).astype(jnp.bfloat16)
    gate_act = jnp.dot(hidden, w_gate, preferred_element_type=jnp.float32)
    up_act = jnp.dot(hidden, w_up, preferred_element_type=jnp.float32)
    swiglu = (jax.nn.silu(gate_act) * up_act).astype(jnp.bfloat16)
    hidden_out = (hidden.astype(jnp.float32) + jnp.dot(swiglu, w_down, preferred_element_type=jnp.float32)).astype(jnp.bfloat16)
    expert_buf = dispatch(hidden, w_router, expert_ids)
    return hidden_out, expert_buf
```

```python
import math
import jax
import jax.numpy as jnp
from jax import lax
from jax.experimental import pallas as pl
from jax.experimental.pallas import tpu as pltpu
from jax.sharding import PartitionSpec as P

MESH = pl.DeviceIdType.MESH
F32 = jnp.float32
BF16 = jnp.bfloat16

HD = 128
D = 2048
HALF = 1024
TOK = 64
CHIP = 128
SEQ = 256
NX = 8
XC = D // NX
NEXP = 15
CAP = 8
SLOTS = 32


def dot(a, b):
    return jnp.dot(a, b, preferred_element_type=F32)


def dot_t(a, b):
    return lax.dot_general(a, b, (((1,), (1,)), ((), ())), preferred_element_type=F32)


def body(x_ref, wq, wk, wv, wo, wg, wu, wd, wr, ids_ref, y_ref, buf_ref,
         x_v, w_v, wo_v, wg_v, wu_v, wd_v, wr_v, ids_v,
         qkv_v, acc_v, o_own, o_oth, hacc_v, h_own, h_oth, ga_v, ua_v, a_own, a_oth, ya_v, y_v,
         wmap_v, p_v, lt_v, gate_v, st_v,
         s_x, s_w, s_w2, s_misc, s_out,
         xi_s, xi_r, xr_s, xr_r, xp_s, xp_r, id_s, id_r, o_s, o_r, h_s, h_r, a_s, a_r):
    dp = lax.axis_index("dp")
    s = lax.axis_index("sp")
    chip = s // 2
    j = s % 2
    partner = chip * 2 + (1 - j)
    remote = (1 - chip) * 2 + j
    diag = (1 - chip) * 2 + (1 - j)
    jo = pl.multiple_of(j * HALF, HALF)
    jn = pl.multiple_of((1 - j) * HALF, HALF)
    r_own = pl.ds(pl.multiple_of(s * TOK, TOK), TOK)
    r_remote = pl.ds(pl.multiple_of(remote * TOK, TOK), TOK)
    r_L = pl.ds(pl.multiple_of(chip * CHIP, CHIP), CHIP)
    r_R = pl.ds(pl.multiple_of((1 - chip) * CHIP, CHIP), CHIP)

    barrier = pltpu.get_barrier_semaphore()
    for p in (partner, remote, diag):
        pl.semaphore_signal(barrier, inc=1, device_id=(dp, p), device_id_type=MESH)

    x_in = pltpu.make_async_copy(x_ref, x_v.at[r_own, :], s_x.at[0])
    x_in.start()
    ids_in = pltpu.make_async_copy(ids_ref, ids_v.at[s], s_x.at[1])
    ids_in.start()
    loads = []
    for i, w in enumerate((wk, wv, wq)):
        for n in range(2):
            c = pltpu.make_async_copy(
                w.at[:, pl.ds(pl.multiple_of(j * HALF + n * 512, 512), 512)],
                w_v.at[i, :, pl.ds(n * 512, 512)], s_w.at[i * 2 + n])
            c.start()
            loads.append(c)
    loads2 = []
    for i, (w, v) in enumerate(((wo, wo_v), (wg, wg_v), (wu, wu_v))):
        for n, off in enumerate((jo, jn)):
            c = pltpu.make_async_copy(w.at[pl.ds(off, HALF), pl.ds(jo, HALF)], v.at[n], s_w2.at[i * 2 + n])
            c.start()
            loads2.append(c)
    for n, off in enumerate((jo, jn)):
        for m, coff in enumerate((jo, jn)):
            c = pltpu.make_async_copy(wd.at[pl.ds(off, HALF), pl.ds(coff, HALF)],
                                      wd_v.at[n, :, pl.ds(m * HALF, HALF)], s_w2.at[6 + n * 2 + m])
            c.start()
            loads2.append(c)
    wr_in = [pltpu.make_async_copy(wr.at[:, pl.ds(off, HALF)], wr_v.at[n], s_misc.at[n]) for n, off in enumerate((jo, jn))]
    for c in wr_in:
        c.start()

    def rcopy(src, dst, ss, rs, p):
        return pltpu.make_async_remote_copy(src_ref=src, dst_ref=dst, send_sem=ss, recv_sem=rs,
                                            device_id=(dp, p), device_id_type=MESH)

    def x_ici(k):
        c = pl.ds(pl.multiple_of(k * XC, XC), XC)
        return rcopy(x_v.at[r_own, c], x_v.at[r_own, c], xi_s.at[k], xi_r.at[k], remote)

    def x_relay(k):
        c = pl.ds(pl.multiple_of(k * XC, XC), XC)
        return rcopy(x_v.at[r_remote, c], x_v.at[r_remote, c], xr_s.at[k], xr_r.at[k], partner)

    pl.semaphore_wait(barrier, 3)
    x_in.wait()
    ids_in.wait()
    x_part = rcopy(x_v.at[r_own, :], x_v.at[r_own, :], xp_s.at[0], xp_r.at[0], partner)
    x_part.start()
    for k in range(NX):
        x_ici(k).start()
    id_copies = [rcopy(ids_v.at[s], ids_v.at[s], id_s.at[n], id_r.at[n], p) for n, p in enumerate((partner, remote, diag))]
    for c in id_copies:
        c.start()

    x_part.wait_recv()
    for i in range(3):
        for n in range(2):
            loads[i * 2 + n].wait()
            qkv_v[i, r_L, n * 512:(n + 1) * 512] = dot(x_v[r_L, :], w_v[i, :, n * 512:(n + 1) * 512]).astype(BF16)

    for c in id_copies:
        c.wait_recv()
    idst = jnp.concatenate([ids_v[t] for t in range(4)], axis=1)
    e_ids = lax.broadcasted_iota(jnp.int32, (16, SEQ), 0) + NEXP * s
    hit = jnp.zeros((16, SEQ), F32)
    for c in range(4):
        hit = jnp.where(idst[c:c + 1, :] == e_ids, 1.0, hit)
    t_row = lax.broadcasted_iota(jnp.int32, (SEQ, SEQ), 0)
    t_col = lax.broadcasted_iota(jnp.int32, (SEQ, SEQ), 1)
    earlier = jnp.where((t_row < t_col) & (t_row // TOK == t_col // TOK), 1.0, 0.0).astype(BF16)
    rank = dot(hit.astype(BF16), earlier)
    src8 = (CAP * (lax.broadcasted_iota(jnp.int32, (16, SEQ), 1) // TOK)).astype(F32)
    wmap = jnp.where((hit > 0.5) & (rank < CAP - 0.5), rank + src8, 99.0)
    wmap_v[...] = wmap
    slot = lax.broadcasted_iota(jnp.int32, (SLOTS, SEQ), 0).astype(F32)
    for e in range(NEXP):
        p_v[e * SLOTS:(e + 1) * SLOTS, :] = jnp.where(wmap[e:e + 1, :] == slot, 1.0, 0.0).astype(BF16)

    acc_v[...] = jnp.zeros_like(acc_v)
    x_ici(0).wait_recv()
    x_relay(0).start()

    def r_step(k, carry):
        x_ici(k + 1).wait_recv()
        x_relay(k + 1).start()
        x_relay(k).wait_recv()
        c = pl.ds(pl.multiple_of(k * XC, XC), XC)
        xr = x_v[r_R, c]
        for i in range(3):
            acc_v[i] += dot(xr, w_v[i, c, :])
        return carry

    lax.fori_loop(0, NX - 1, r_step, 0)
    x_relay(NX - 1).wait_recv()
    xr = x_v[r_R, D - XC:]
    for i in range(3):
        qkv_v[i, r_R, :] = (acc_v[i] + dot(xr, w_v[i, D - XC:, :])).astype(BF16)

    scale = 1.0 / math.sqrt(HD)
    tri = lax.broadcasted_iota(jnp.int32, (CHIP, CHIP), 0) >= lax.broadcasted_iota(jnp.int32, (CHIP, CHIP), 1)
    o_copies = []
    for hd in range(8):
        c = slice(hd * HD, (hd + 1) * HD)
        k_h, v_h, q_h = qkv_v[0, :, c], qkv_v[1, :, c], qkv_v[2, :, c]
        sc = dot_t(q_h, k_h) * scale
        top = jnp.where(tri, sc[:CHIP, :CHIP], -jnp.inf)
        bot0 = sc[CHIP:, :CHIP]
        bot1 = jnp.where(tri, sc[CHIP:, CHIP:], -jnp.inf)
        e_top = jnp.exp(top - jnp.max(top, axis=1, keepdims=True))
        p_top = (e_top * (1.0 / jnp.sum(e_top, axis=1, keepdims=True))).astype(BF16)
        m_bot = jnp.max(jnp.maximum(bot0, bot1), axis=1, keepdims=True)
        e0, e1 = jnp.exp(bot0 - m_bot), jnp.exp(bot1 - m_bot)
        inv = 1.0 / jnp.sum(e0 + e1, axis=1, keepdims=True)
        p_bot = jnp.concatenate([(e0 * inv).astype(BF16), (e1 * inv).astype(BF16)], axis=1)
        o_own[:CHIP, c] = dot(p_top, v_h[:CHIP]).astype(BF16)
        o_own[CHIP:, c] = dot(p_bot, v_h).astype(BF16)
        if hd % 2 == 1:
            n = hd // 2
            cc = slice(n * 256, (n + 1) * 256)
            cp = rcopy(o_own.at[:, cc], o_oth.at[:, cc], o_s.at[n], o_r.at[n], partner)
            cp.start()
            o_copies.append(cp)

    loads2[0].wait()
    loads2[1].wait()
    hacc_v[...] = dot(o_own[...], wo_v[0])
    for cp in o_copies:
        cp.wait_recv()
    h_copies = []
    for n in range(4):
        cc = slice(n * 256, (n + 1) * 256)
        xc = x_v[:, pl.ds(pl.multiple_of(j * HALF + n * 256, 256), 256)].astype(F32)
        h_own[:, cc] = (xc + (hacc_v[:, cc] + dot(o_oth[...], wo_v[1, :, cc]))).astype(BF16)
        cp = rcopy(h_own.at[:, cc], h_oth.at[:, cc], h_s.at[n], h_r.at[n], partner)
        cp.start()
        h_copies.append(cp)

    for c in loads2[2:6]:
        c.wait()
    ga_v[...] = dot(h_own[r_L, :], wg_v[0])
    ua_v[...] = dot(h_own[r_L, :], wu_v[0])
    for cp in h_copies:
        cp.wait_recv()
    a_copies = []
    r_mine = pl.ds(pl.multiple_of(j * TOK, TOK), TOK)
    r_his = pl.ds(pl.multiple_of((1 - j) * TOK, TOK), TOK)
    for n in range(4):
        cc = slice(n * 256, (n + 1) * 256)
        g = ga_v[:, cc] + dot(h_oth[r_L, :], wg_v[1, :, cc])
        u = ua_v[:, cc] + dot(h_oth[r_L, :], wu_v[1, :, cc])
        a_own[:, cc] = (jax.nn.silu(g) * u).astype(BF16)
        cp = rcopy(a_own.at[r_his, cc], a_oth.at[:, cc], a_s.at[n], a_r.at[n], partner)
        cp.start()
        a_copies.append(cp)

    for c in wr_in:
        c.wait()
    logits = dot_t(h_own[...], wr_v[0]) + dot_t(h_oth[...], wr_v[1])
    lt_v[...] = jax.nn.sigmoid(logits.T)
    for e in range(NEXP):
        g_row = lt_v[pl.ds(NEXP * s + e, 1), :]
        picked = jnp.where(wmap_v[e:e + 1, :] == slot, g_row, 0.0)
        gate_v[e * SLOTS:(e + 1) * SLOTS, :] = jnp.broadcast_to(jnp.sum(picked, axis=1, keepdims=True), (SLOTS, HD))
    outs = []
    for m, (h, off) in enumerate(((h_own, jo), (h_oth, jn))):
        for n in range(4):
            cc = slice(n * 256, (n + 1) * 256)
            rows = dot(p_v[...], h[:, cc])
            gate = gate_v[...]
            st_v[m, :, cc] = (rows * jnp.concatenate([gate, gate], axis=1)).astype(BF16)
        cp = pltpu.make_async_copy(st_v.at[m], buf_ref.at[:, pl.ds(off, HALF)], s_out.at[m])
        cp.start()
        outs.append(cp)

    for c in loads2[6:]:
        c.wait()
    ya_v[...] = dot(a_own[r_mine, :], wd_v[0])
    for cp in a_copies:
        cp.wait_recv()
    for m, (h, off) in enumerate(((h_own, jo), (h_oth, jn))):
        cc = slice(m * HALF, (m + 1) * HALF)
        part = ya_v[:, cc] + dot(a_oth[...], wd_v[1, :, cc])
        y_v[:, cc] = (h[r_own, :].astype(F32) + part).astype(BF16)
        cp = pltpu.make_async_copy(y_v.at[:, cc], y_ref.at[:, pl.ds(off, HALF)], s_out.at[2 + m])
        cp.start()
        outs.append(cp)

    x_part.wait_send()
    for k in range(NX):
        x_ici(k).wait_send()
        x_relay(k).wait_send()
    for cp in id_copies + o_copies + h_copies + a_copies:
        cp.wait_send()
    for cp in outs:
        cp.wait()


def fused(x, wq, wk, wv, wo, wg, wu, wd, wr, ids):
    hbm = pl.BlockSpec(memory_space=pltpu.HBM)
    v = pltpu.VMEM
    dma = pltpu.SemaphoreType.DMA
    return pl.pallas_call(
        body,
        out_shape=(jax.ShapeDtypeStruct((TOK, D), BF16), jax.ShapeDtypeStruct((NEXP * SLOTS, D), BF16)),
        in_specs=[hbm] * 10,
        out_specs=(hbm, hbm),
        scratch_shapes=[
            v((SEQ, D), BF16), v((3, D, HALF), BF16), v((2, HALF, HALF), BF16), v((2, HALF, HALF), BF16),
            v((2, HALF, HALF), BF16), v((2, HALF, D), BF16), v((2, 60, HALF), BF16), v((4, 4, TOK), jnp.int32),
            v((3, SEQ, HALF), BF16), v((3, CHIP, HALF), F32), v((SEQ, HALF), BF16), v((SEQ, HALF), BF16),
            v((SEQ, HALF), F32), v((SEQ, HALF), BF16), v((SEQ, HALF), BF16), v((CHIP, HALF), F32),
            v((CHIP, HALF), F32), v((CHIP, HALF), BF16), v((TOK, HALF), BF16), v((TOK, D), F32), v((TOK, D), BF16),
            v((16, SEQ), F32), v((NEXP * SLOTS, SEQ), BF16), v((60, SEQ), F32), v((NEXP * SLOTS, HD), F32),
            v((2, NEXP * SLOTS, HALF), BF16),
            dma((2,)), dma((6,)), dma((10,)), dma((2,)), dma((4,)),
            dma((NX,)), dma((NX,)), dma((NX,)), dma((NX,)), dma((1,)), dma((1,)), dma((3,)), dma((3,)),
            dma((4,)), dma((4,)), dma((4,)), dma((4,)), dma((4,)), dma((4,)),
        ],
        compiler_params=pltpu.CompilerParams(collective_id=0, has_side_effects=True,
                                             vmem_limit_bytes=60 * 1024 * 1024),
        cost_estimate=pl.CostEstimate(flops=6_000_000_000, bytes_accessed=36_000_000, transcendentals=600_000),
        name="fused_block",
    )(x, wq, wk, wv, wo, wg, wu, wd, wr, ids)


def solution(mesh):
    row_spec = P(('dp', 'sp'), None)
    buf_spec = P(('dp', 'sp'), None, None)
    replicated = P()

    def local_step(tokens, w_query, w_key, w_value, w_out, w_gate, w_up, w_down, w_router, expert_ids):
        y, buf = fused(tokens, w_query, w_key, w_value, w_out, w_gate, w_up, w_down, w_router.T, expert_ids.T)
        return y, buf.reshape(NEXP, SLOTS, D)

    return jax.shard_map(local_step, mesh=mesh, in_specs=(row_spec,) + (replicated,) * 8 + (row_spec,),
                         out_specs=(row_spec, buf_spec), check_vma=False)
```

```python
import math
import jax
import jax.numpy as jnp
from jax import lax
from jax.experimental import pallas as pl
from jax.experimental.pallas import tpu as pltpu
from jax.sharding import PartitionSpec as P

MESH = pl.DeviceIdType.MESH
F32 = jnp.float32
BF16 = jnp.bfloat16

HD = 128
D = 2048
HALF = 1024
TOK = 64
CHIP = 128
SEQ = 256
NX = 8
XC = D // NX
NEXP = 15
CAP = 8
SLOTS = 32


def dot(a, b):
    return jnp.dot(a, b, preferred_element_type=F32)


def dot_t(a, b):
    return lax.dot_general(a, b, (((1,), (1,)), ((), ())), preferred_element_type=F32)


def body(x_ref, wq, wk, wv, wo, wg, wu, wd, wr, ids_ref, y_ref, buf_ref,
         x_v, w_v, wo_v, wg_v, wu_v, wd_v, wr_v, ids_v,
         qkv_v, acc_v, o_own, o_oth, hacc_v, h_own, h_oth, ga_v, ua_v, a_own, a_oth, ya_v,
         wmap_v, p_v, lt_v, gate_v,
         s_x, s_w, s_w2, s_misc,
         xi_s, xi_r, xr_s, xr_r, xp_s, xp_r, id_s, id_r, o_s, o_r, h_s, h_r, a_s, a_r):
    dp = lax.axis_index("dp")
    s = lax.axis_index("sp")
    chip = s // 2
    j = s % 2
    partner = chip * 2 + (1 - j)
    remote = (1 - chip) * 2 + j
    diag = (1 - chip) * 2 + (1 - j)
    jo = pl.multiple_of(j * HALF, HALF)
    jn = pl.multiple_of((1 - j) * HALF, HALF)
    r_own = pl.ds(pl.multiple_of(s * TOK, TOK), TOK)
    r_remote = pl.ds(pl.multiple_of(remote * TOK, TOK), TOK)
    r_L = pl.ds(pl.multiple_of(chip * CHIP, CHIP), CHIP)
    r_R = pl.ds(pl.multiple_of((1 - chip) * CHIP, CHIP), CHIP)

    barrier = pltpu.get_barrier_semaphore()
    for p in (partner, remote, diag):
        pl.semaphore_signal(barrier, inc=1, device_id=(dp, p), device_id_type=MESH)

    def rcopy(src, dst, ss, rs, p):
        return pltpu.make_async_remote_copy(src_ref=src, dst_ref=dst, send_sem=ss, recv_sem=rs,
                                            device_id=(dp, p), device_id_type=MESH)

    def x_ici(k):
        c = pl.ds(pl.multiple_of(k * XC, XC), XC)
        return rcopy(x_v.at[r_own, c], x_v.at[r_own, c], xi_s.at[k], xi_r.at[k], remote)

    def x_relay(k):
        c = pl.ds(pl.multiple_of(k * XC, XC), XC)
        return rcopy(x_v.at[r_remote, c], x_v.at[r_remote, c], xr_s.at[k], xr_r.at[k], partner)

    x_in = pltpu.make_async_copy(x_ref, x_v.at[r_own, :], s_x.at[0])
    x_in.start()
    ids_in = pltpu.make_async_copy(ids_ref, ids_v.at[s], s_x.at[1])
    ids_in.start()
    x_in.wait()
    ids_in.wait()
    pl.semaphore_wait(barrier, 3)
    id_copies = [rcopy(ids_v.at[s], ids_v.at[s], id_s.at[n], id_r.at[n], p) for n, p in enumerate((partner, remote, diag))]
    for c in id_copies:
        c.start()
    x_part = rcopy(x_v.at[r_own, :], x_v.at[r_own, :], xp_s.at[0], xp_r.at[0], partner)
    x_part.start()
    for k in range(NX):
        x_ici(k).start()

    loads = []
    for i, w in enumerate((wk, wv, wq)):
        for n in range(2):
            c = pltpu.make_async_copy(
                w.at[:, pl.ds(pl.multiple_of(j * HALF + n * 512, 512), 512)],
                w_v.at[i, :, pl.ds(n * 512, 512)], s_w.at[i * 2 + n])
            c.start()
            loads.append(c)
    loads2 = []
    for i, (w, v) in enumerate(((wo, wo_v), (wg, wg_v), (wu, wu_v))):
        for n, off in enumerate((jo, jn)):
            loads2.append(pltpu.make_async_copy(w.at[pl.ds(off, HALF), pl.ds(jo, HALF)], v.at[n], s_w2.at[i * 2 + n]))
    for n, off in enumerate((jo, jn)):
        for m, coff in enumerate((jo, jn)):
            loads2.append(pltpu.make_async_copy(wd.at[pl.ds(off, HALF), pl.ds(coff, HALF)],
                                                wd_v.at[n, :, pl.ds(m * HALF, HALF)], s_w2.at[6 + n * 2 + m]))
    wr_in = [pltpu.make_async_copy(wr.at[:, pl.ds(off, HALF)], wr_v.at[n], s_misc.at[n]) for n, off in enumerate((jo, jn))]

    x_part.wait_recv()
    for i in range(3):
        for n in range(2):
            loads[i * 2 + n].wait()
            qkv_v[i, r_L, n * 512:(n + 1) * 512] = dot(x_v[r_L, :], w_v[i, :, n * 512:(n + 1) * 512]).astype(BF16)
            k = i * 2 + n - 2
            if k >= 0:
                x_ici(k).wait_recv()
                x_relay(k).start()
    for c in loads2[:2] + wr_in + loads2[2:]:
        c.start()

    for c in id_copies:
        c.wait_recv()
    idst = jnp.concatenate([ids_v[t] for t in range(4)], axis=1)
    e_ids = lax.broadcasted_iota(jnp.int32, (16, SEQ), 0) + NEXP * s
    hit = jnp.zeros((16, SEQ), F32)
    for c in range(4):
        hit = jnp.where(idst[c:c + 1, :] == e_ids, 1.0, hit)
    t_row = lax.broadcasted_iota(jnp.int32, (SEQ, SEQ), 0)
    t_col = lax.broadcasted_iota(jnp.int32, (SEQ, SEQ), 1)
    earlier = jnp.where((t_row < t_col) & (t_row // TOK == t_col // TOK), 1.0, 0.0).astype(BF16)
    rank = dot(hit.astype(BF16), earlier)
    src8 = (CAP * (lax.broadcasted_iota(jnp.int32, (16, SEQ), 1) // TOK)).astype(F32)
    wmap = jnp.where((hit > 0.5) & (rank < CAP - 0.5), rank + src8, 99.0)
    wmap_v[...] = wmap
    slot = lax.broadcasted_iota(jnp.int32, (SLOTS, SEQ), 0).astype(F32)
    for e in range(NEXP):
        p_v[e * SLOTS:(e + 1) * SLOTS, :] = jnp.where(wmap[e:e + 1, :] == slot, 1.0, 0.0).astype(BF16)

    for k in range(NX):
        if k + 2 >= 4 and k + 2 < NX:
            x_ici(k + 2).wait_recv()
            x_relay(k + 2).start()
        x_relay(k).wait_recv()
        c = slice(k * XC, (k + 1) * XC)
        xr = x_v[r_R, c]
        for i in range(3):
            part = dot(xr, w_v[i, c, :])
            if k == 0:
                acc_v[i] = part
            elif k < NX - 1:
                acc_v[i] += part
            else:
                qkv_v[i, r_R, :] = (acc_v[i] + part).astype(BF16)

    scale = 1.0 / math.sqrt(HD)
    tri = lax.broadcasted_iota(jnp.int32, (CHIP, CHIP), 0) >= lax.broadcasted_iota(jnp.int32, (CHIP, CHIP), 1)
    def scores(hd):
        c = slice(hd * HD, (hd + 1) * HD)
        return dot_t(qkv_v[2, :, c], qkv_v[0, :, c])

    def probs(sc):
        sc = sc * scale
        top = jnp.where(tri, sc[:CHIP, :CHIP], -jnp.inf)
        bot0 = sc[CHIP:, :CHIP]
        bot1 = jnp.where(tri, sc[CHIP:, CHIP:], -jnp.inf)
        e_top = jnp.exp(top - jnp.max(top, axis=1, keepdims=True))
        p_top = (e_top * (1.0 / jnp.sum(e_top, axis=1, keepdims=True))).astype(BF16)
        m_bot = jnp.max(jnp.maximum(bot0, bot1), axis=1, keepdims=True)
        e0, e1 = jnp.exp(bot0 - m_bot), jnp.exp(bot1 - m_bot)
        inv = 1.0 / jnp.sum(e0 + e1, axis=1, keepdims=True)
        return p_top, jnp.concatenate([(e0 * inv).astype(BF16), (e1 * inv).astype(BF16)], axis=1)

    def weighted(hd, p):
        c = slice(hd * HD, (hd + 1) * HD)
        v_h = qkv_v[1, :, c]
        o_own[:CHIP, c] = dot(p[0], v_h[:CHIP]).astype(BF16)
        o_own[CHIP:, c] = dot(p[1], v_h).astype(BF16)

    o_copies = []
    for n in range(2):
        heads = range(n * 4, n * 4 + 4)
        sc = [scores(hd) for hd in heads]
        pr = [probs(t) for t in sc]
        for hd, p in zip(heads, pr):
            weighted(hd, p)
        cc = slice(n * 512, (n + 1) * 512)
        cp = rcopy(o_own.at[:, cc], o_oth.at[:, cc], o_s.at[n], o_r.at[n], partner)
        cp.start()
        o_copies.append(cp)

    loads2[0].wait()
    loads2[1].wait()
    hacc_v[...] = dot(o_own[...], wo_v[0])
    for cp in o_copies:
        cp.wait_recv()
    h_copies = []
    for n in range(2):
        cc = slice(n * 512, (n + 1) * 512)
        xc = x_v[:, pl.ds(pl.multiple_of(j * HALF + n * 512, 512), 512)].astype(F32)
        h_own[:, cc] = (xc + (hacc_v[:, cc] + dot(o_oth[...], wo_v[1, :, cc]))).astype(BF16)
        cp = rcopy(h_own.at[:, cc], h_oth.at[:, cc], h_s.at[n], h_r.at[n], partner)
        cp.start()
        h_copies.append(cp)

    for c in loads2[2:6]:
        c.wait()
    ga_v[...] = dot(h_own[r_L, :], wg_v[0])
    ua_v[...] = dot(h_own[r_L, :], wu_v[0])
    for cp in h_copies:
        cp.wait_recv()
    a_copies = []
    r_mine = pl.ds(pl.multiple_of(j * TOK, TOK), TOK)
    r_his = pl.ds(pl.multiple_of((1 - j) * TOK, TOK), TOK)
    for n in range(2):
        cc = slice(n * 512, (n + 1) * 512)
        g = ga_v[:, cc] + dot(h_oth[r_L, :], wg_v[1, :, cc])
        u = ua_v[:, cc] + dot(h_oth[r_L, :], wu_v[1, :, cc])
        a_own[:, cc] = (jax.nn.silu(g) * u).astype(BF16)
        cp = rcopy(a_own.at[r_his, cc], a_oth.at[:, cc], a_s.at[n], a_r.at[n], partner)
        cp.start()
        a_copies.append(cp)

    for c in wr_in:
        c.wait()
    logits = dot_t(h_own[...], wr_v[0]) + dot_t(h_oth[...], wr_v[1])
    lt_v[...] = jax.nn.sigmoid(logits.T)
    for e in range(NEXP):
        g_row = lt_v[pl.ds(NEXP * s + e, 1), :]
        picked = jnp.where(wmap_v[e:e + 1, :] == slot, g_row, 0.0)
        gate_v[e * SLOTS:(e + 1) * SLOTS, :] = jnp.broadcast_to(jnp.sum(picked, axis=1, keepdims=True), (SLOTS, HD))
    for h, first in ((h_own, j), (h_oth, 1 - j)):
        for n in range(4):
            rows = dot(p_v[...], h[:, n * 256:(n + 1) * 256])
            gate = gate_v[...]
            buf_ref[:, pl.ds(pl.multiple_of(first * HALF + n * 256, 256), 256)] = (
                rows * jnp.concatenate([gate, gate], axis=1)).astype(BF16)

    for c in loads2[6:]:
        c.wait()
    ya_v[...] = dot(a_own[r_mine, :], wd_v[0])
    for cp in a_copies:
        cp.wait_recv()
    for m, (h, off) in enumerate(((h_own, jo), (h_oth, jn))):
        cc = slice(m * HALF, (m + 1) * HALF)
        part = ya_v[:, cc] + dot(a_oth[...], wd_v[1, :, cc])
        y_ref[:, pl.ds(off, HALF)] = (h[r_own, :].astype(F32) + part).astype(BF16)

    x_part.wait_send()
    for k in range(NX):
        x_ici(k).wait_send()
        x_relay(k).wait_send()
    for cp in id_copies + o_copies + h_copies + a_copies:
        cp.wait_send()


def fused(x, wq, wk, wv, wo, wg, wu, wd, wr, ids):
    hbm = pl.BlockSpec(memory_space=pltpu.HBM)
    v = pltpu.VMEM
    dma = pltpu.SemaphoreType.DMA
    return pl.pallas_call(
        body,
        out_shape=(v((TOK, D), BF16), v((NEXP * SLOTS, D), BF16)),
        in_specs=[hbm] * 10,
        out_specs=(pl.BlockSpec(memory_space=v),) * 2,
        scratch_shapes=[
            v((SEQ, D), BF16), v((3, D, HALF), BF16), v((2, HALF, HALF), BF16), v((2, HALF, HALF), BF16),
            v((2, HALF, HALF), BF16), v((2, HALF, D), BF16), v((2, 60, HALF), BF16), v((4, 4, TOK), jnp.int32),
            v((3, SEQ, HALF), BF16), v((3, CHIP, HALF), F32), v((SEQ, HALF), BF16), v((SEQ, HALF), BF16),
            v((SEQ, HALF), F32), v((SEQ, HALF), BF16), v((SEQ, HALF), BF16), v((CHIP, HALF), F32),
            v((CHIP, HALF), F32), v((CHIP, HALF), BF16), v((TOK, HALF), BF16), v((TOK, D), F32),
            v((16, SEQ), F32), v((NEXP * SLOTS, SEQ), BF16), v((60, SEQ), F32), v((NEXP * SLOTS, HD), F32),
            dma((2,)), dma((6,)), dma((10,)), dma((2,)),
            dma((NX,)), dma((NX,)), dma((NX,)), dma((NX,)), dma((1,)), dma((1,)), dma((3,)), dma((3,)),
            dma((2,)), dma((2,)), dma((2,)), dma((2,)), dma((2,)), dma((2,)),
        ],
        compiler_params=pltpu.CompilerParams(collective_id=0, has_side_effects=True,
                                             vmem_limit_bytes=60 * 1024 * 1024),
        cost_estimate=pl.CostEstimate(flops=6_000_000_000, bytes_accessed=36_000_000, transcendentals=600_000),
        name="fused_block",
    )(x, wq, wk, wv, wo, wg, wu, wd, wr, ids)


def solution(mesh):
    row_spec = P(('dp', 'sp'), None)
    buf_spec = P(('dp', 'sp'), None, None)
    replicated = P()

    def local_step(tokens, w_query, w_key, w_value, w_out, w_gate, w_up, w_down, w_router, expert_ids):
        y, buf = fused(tokens, w_query, w_key, w_value, w_out, w_gate, w_up, w_down, w_router.T, expert_ids.T)
        return y, buf.reshape(NEXP, SLOTS, D)

    return jax.shard_map(local_step, mesh=mesh, in_specs=(row_spec,) + (replicated,) * 8 + (row_spec,),
                         out_specs=(row_spec, buf_spec), check_vma=False)
```
